32 devices in a mesh: replica: 8 (over y, x, core), shard: 4 (over z).
Axes of the slice: x: 2, y: 2, z: 4, core: 2. Of those that a mesh axis runs over, the one named last changes fastest.
Arguments:
- params: float32 [8, 64, 28672], P('replica', 'shard'), may hold values from -6 to 6
- first_moment: float32 [8, 64, 28672], P('replica', 'shard'), may hold values from -3 to 3
- second_moment: float32 [8, 64, 28672], P('replica', 'shard'), may hold values from 0.25 to 4
- grads: bfloat16 [4, 8, 64, 28672], P(None, 'replica', 'shard'), may hold values from -6 to 6
- push_weight: float32 [8], P('replica'), may hold values from 0.5 to 2
Outputs:
- final_weights: bfloat16 [8, 64, 28672], P('replica')
The draws below stay inside these ranges and needn't reach their ends.
All inputs are finite; a program needn't handle non-finite values.
Results may differ from the reference program's by a relative error of at most 0.001.
Values may be sent and summed in bfloat16 or wider, within the bound.
A program may use at most 64 MiB of HBM per device.

```python
import math
import jax
import jax.numpy as jnp

COLS = 28672
STEPS = 4
ROWS = 64
REPLICAS = 8


def steps_of(key, shape, pieces, low, top_value):
    level, own = 1.0, jax.random.fold_in(key, 6)
    for dim, blocks in pieces:
        draws = jnp.exp(jax.random.uniform(jax.random.fold_in(own, dim), (blocks,), jnp.float32, low / len(pieces), top_value / len(pieces)))
        level = level * jnp.repeat(draws, shape[dim] // blocks).reshape([-1 if axis == dim else 1 for axis in range(len(shape))])
    return level


def scatter_about(key, dims, spread, most, cuts=(), held_as=jnp.bfloat16):
    level = steps_of(key, dims, cuts, -0.22, 0.18) if cuts else 1.0
    array = jax.random.normal(key, dims, jnp.float32) * spread * level
    return jnp.minimum(jnp.maximum(array, -most), most).astype(held_as)


def setup_inputs(seed: int = 0) -> dict:
    key_list = jax.random.split(jax.random.key(seed), 6)
    return {
        "params": scatter_about(key_list[0], (REPLICAS, ROWS, COLS), 1.0, 6.0, ((0, 8), (1, 4)), jnp.float32),
        "first_moment": scatter_about(key_list[1], (REPLICAS, ROWS, COLS), 0.5, 3.0, ((0, 8), (1, 4)), jnp.float32),
        "second_moment": jnp.clip(jnp.exp(math.log(4.0) - 2.7725887 * jax.random.uniform(key_list[2], (REPLICAS, ROWS, COLS), jnp.float32) ** steps_of(key_list[2], (REPLICAS, ROWS, COLS), ((0, 8), (1, 4)), -0.2, 0.2)), 0.25, 4.0),
        "grads": scatter_about(key_list[3], (STEPS, REPLICAS, ROWS, COLS), 1.0, 6.0, ((1, 8), (2, 4))),
        "push_weight": jnp.clip(0.5 + 1.5 * jax.random.uniform(key_list[4], (REPLICAS,), jnp.float32) ** steps_of(key_list[4], (REPLICAS,), ((0, 8),), -0.2, 0.2), 0.5, 2.0),
    }


beta_one = 0.9
beta_two = 0.95
learn_rate = 0.1
decay_rate = 0.1
epsilon = 1e-08
adam_offset = 101

def reference(params, first_moment, second_moment, grads, push_weight):
    levels = REPLICAS.bit_length() - 1
    weight = push_weight
    numer = params * weight[:, None, None]
    for iteration in range(STEPS):
        distance = 2 ** (iteration % levels)
        count = adam_offset + iteration
        first_fix = 1.0 - beta_one ** count
        second_fix = 1.0 - beta_two ** count
        current = numer / weight[:, None, None]
        gradient = grads[iteration].astype(jnp.float32)
        first_moment = beta_one * first_moment + (1.0 - beta_one) * gradient
        second_moment = beta_two * second_moment + (1.0 - beta_two) * gradient * gradient
        update = first_moment / first_fix / (jnp.sqrt(second_moment / second_fix) + epsilon)
        current = current - learn_rate * (update + decay_rate * current)
        numer = current * weight[:, None, None]
        numer = 0.5 * numer + 0.5 * jnp.roll(numer, distance, axis=0)
        weight = 0.5 * weight + 0.5 * jnp.roll(weight, distance, axis=0)
    return (numer / weight[:, None, None]).astype(jnp.bfloat16)
```

```python
import functools

import jax
import jax.numpy as jnp
from jax import lax
from jax.experimental import pallas as pl
from jax.experimental.pallas import tpu as pltpu
from jax.sharding import PartitionSpec as P

STEPS = 4


beta_one = 0.9
beta_two = 0.95
learn_rate = 0.1
decay_rate = 0.1
epsilon = 1e-08
adam_offset = 101

CODE_SCALE = 8.0
LAG = 2
CHUNKS = 28
MESH = pl.DeviceIdType.MESH


def plan_of(replicas):
    levels = replicas.bit_length() - 1
    distances = [2 ** (step % levels) for step in range(STEPS)]
    every = {2**level for level in range(levels)}
    plan = []
    for step, distance in enumerate(distances):
        later = set(distances[step + 1 :])
        if every <= later:
            continue
        above = {d for d in every if d > distance}
        plan.append((step, distance, above <= later))
    return plan


def encode(value):
    power = value * CODE_SCALE
    power = power * power
    power = power * power
    power = power * power
    power = power * power
    return jnp.where(value < 0.0, -power, power).astype(jnp.bfloat16)


def decode(code):
    code = code.astype(jnp.float32)
    size = jnp.exp(jnp.log(jnp.abs(code)) * (1.0 / 16.0)) * (1.0 / CODE_SCALE)
    return jnp.where(code < 0.0, -size, size)


def kernel(
    plan, replicas, shards, chunks, chunk, sub,
    params_ref, first_ref, second_ref, grads_ref, weight_ref, out_ref,
    params, first, second, grads, weights, scales, acc, terms, sent, arrived, final,
    load_sem, wsend, wrecv, xsend, xrecv, zsend, zrecv, own_sem,
):
    me, z = lax.axis_index("replica"), lax.axis_index("shard")
    rows = params.shape[0]
    rounds = len(plan)
    keep = 1.0 - learn_rate * decay_rate

    def columns(i):
        return pl.ds(pl.multiple_of(i * chunk, chunk), chunk)

    def slab(index):
        return pl.ds(pl.multiple_of(index * rows, rows), rows)

    def peer(offset):
        return lax.rem(me + offset + replicas, replicas)

    barrier = pltpu.get_barrier_semaphore()
    for k in range(1, replicas):
        pl.semaphore_signal(barrier, inc=1, device_id={"replica": peer(k)}, device_id_type=MESH)

    @pl.when(z > 0)
    def _():
        pl.semaphore_signal(barrier, inc=1, device_id={"shard": z - 1}, device_id_type=MESH)

    @pl.when(z < shards - 1)
    def _():
        pl.semaphore_signal(barrier, inc=1, device_id={"shard": z + 1}, device_id_type=MESH)

    def loads(i):
        cols = columns(i)
        return (
            pltpu.make_async_copy(params_ref.at[0, :, cols], params.at[:, cols], load_sem.at[0, i]),
            pltpu.make_async_copy(first_ref.at[0, :, cols], first.at[:, cols], load_sem.at[1, i]),
            pltpu.make_async_copy(second_ref.at[0, :, cols], second.at[:, cols], load_sem.at[2, i]),
            pltpu.make_async_copy(grads_ref.at[:, 0, :, cols], grads.at[:, :, cols], load_sem.at[3, i]),
        )

    @pl.loop(0, chunks)
    def _(i):
        for copy in loads(i):
            copy.start()

    weights[me] = jnp.full(weights.shape[1:], weight_ref[0], jnp.float32)
    ends_of_line = jnp.where(z > 0, 1, 0) + jnp.where(z < shards - 1, 1, 0)
    pl.semaphore_wait(barrier, replicas - 1 + ends_of_line)

    def weight_copy(k, owner):
        return pltpu.make_async_remote_copy(
            src_ref=weights.at[owner], dst_ref=weights.at[owner],
            send_sem=wsend.at[k - 1], recv_sem=wrecv.at[k - 1],
            device_id={"replica": peer(k)}, device_id_type=MESH,
        )

    for k in range(1, replicas):
        weight_copy(k, me).start()
    for k in range(1, replicas):
        weight_copy(k, peer(-k)).wait_recv()

    def wide(tile):
        tile = jnp.concatenate([tile] * (rows // tile.shape[0]), axis=0) if rows > tile.shape[0] else tile[:rows]
        return jnp.concatenate([tile] * (sub // tile.shape[1]), axis=1)

    levels = replicas.bit_length() - 1
    behind = [weights[peer(-k)] for k in range(replicas)]
    ends = [step for step, _, _ in plan]
    for step in range(STEPS):
        end = min(e for e in ends if e >= step)
        if step == 0:
            scales[0] = wide(behind[0] * keep ** (end + 1))
        scales[1 + step] = wide(behind[0] * (learn_rate * keep ** (end - step)))
        distance = 2 ** (step % levels)
        behind = [0.5 * behind[k] + 0.5 * behind[(k + distance) % replicas] for k in range(replicas)]
    scales[1 + STEPS] = wide(0.5 / behind[0])

    def exchange(k, i):
        _, distance, swap = plan[k]
        if swap:
            to = me + distance - 2 * distance * lax.rem(me // distance, 2)
        else:
            to = peer(distance)
        cols = columns(i)
        return pltpu.make_async_remote_copy(
            src_ref=sent.at[k, :, cols], dst_ref=arrived.at[k, :, cols],
            send_sem=xsend.at[k, i], recv_sem=xrecv.at[k, i],
            device_id={"replica": to}, device_id_type=MESH,
        )

    def gather(way, hop, i):
        sign = 1 - 2 * way
        cols, index = columns(i), z - sign * hop
        target = out_ref.at[0, slab(index), cols]
        return pltpu.make_async_remote_copy(
            src_ref=final.at[:, cols] if hop == 0 else target, dst_ref=target,
            send_sem=zsend.at[way, hop, i], recv_sem=zrecv.at[way, hop, i],
            device_id={"shard": z + sign}, device_id_type=MESH,
        )

    def gathered(way, hop, i):
        sign = 1 - 2 * way
        target = out_ref.at[0, slab(z - sign * hop), columns(i)]
        return pltpu.make_async_remote_copy(
            src_ref=target, dst_ref=target,
            send_sem=zsend.at[way, hop - 1, i], recv_sem=zrecv.at[way, hop - 1, i],
            device_id={"shard": z - sign}, device_id_type=MESH,
        )

    def has_source(way, hop):
        return z >= hop if way == 0 else z + hop < shards

    def has_target(way):
        return z < shards - 1 if way == 0 else z > 0

    def own(i):
        cols = columns(i)
        return pltpu.make_async_copy(final.at[:, cols], out_ref.at[0, slab(z), cols], own_sem.at[i])

    def start_round(i):
        for copy in loads(i):
            copy.wait()
        for j in range(chunk // sub):
            cols = pl.ds(pl.multiple_of(i * chunk + j * sub, sub), sub)
            m, v = first[:, cols], second[:, cols]
            total = scales[0] * params[:, cols]
            k = 0
            for step in range(STEPS):
                g = grads[step, :, cols].astype(jnp.float32)
                count = adam_offset + step
                m = beta_one * m + (1.0 - beta_one) * g
                v = beta_two * v + (1.0 - beta_two) * g * g
                fixed = jnp.sqrt(v * (1.0 / (1.0 - beta_two**count))) + epsilon
                update = m * (1.0 / (1.0 - beta_one**count)) / fixed * scales[1 + step]
                total = -update if total is None else total - update
                if step == ends[k]:
                    if k == 0:
                        acc[:, cols] = total
                        sent[0, :, cols] = encode(total)
                    else:
                        terms[k - 1, :, cols] = total
                    total, k = None, k + 1
        exchange(0, i).start()

    def next_round(k, i):
        exchange(k - 1, i).wait_recv()
        for j in range(chunk // sub):
            cols = pl.ds(pl.multiple_of(i * chunk + j * sub, sub), sub)
            both = acc[:, cols] + decode(arrived[k - 1, :, cols])
            if k < rounds:
                both = both * (0.5 * keep ** (ends[k] - ends[k - 1])) + terms[k - 1, :, cols]
                acc[:, cols] = both
                sent[k, :, cols] = encode(both)
            else:
                final[:, cols] = (both * scales[1 + STEPS]).astype(jnp.bfloat16)
        if k < rounds:
            exchange(k, i).start()
        else:
            for way in range(2):
                pl.when(has_target(way))(lambda way=way: gather(way, 0, i).start())
            own(i).start()

    def pass_on(hop, i):
        for way in range(2):

            @pl.when(jnp.logical_and(has_target(way), has_source(way, hop)))
            def _(way=way):
                gathered(way, hop, i).wait_recv()
                gather(way, hop, i).start()

    hops = shards - 2

    @pl.loop(0, chunks + (rounds + max(hops, 0)) * LAG)
    def _(t):
        def at(stage, act):
            i = t - stage * LAG

            @pl.when(jnp.logical_and(i >= 0, i < chunks))
            def _():
                act(i)

        at(0, start_round)
        for k in range(1, rounds + 1):
            at(k, functools.partial(next_round, k))
        for hop in range(1, hops + 1):
            at(rounds + hop, functools.partial(pass_on, hop))

    for k in range(1, replicas):
        weight_copy(k, me).wait_send()

    @pl.loop(0, chunks)
    def _(i):
        for k in range(rounds):
            exchange(k, i).wait_send()
        own(i).wait()
        for way in range(2):
            for hop in range(shards - 1):

                @pl.when(jnp.logical_and(has_target(way), has_source(way, hop)))
                def _(way=way, hop=hop):
                    gather(way, hop, i).wait_send()

            for hop in range(1, shards):
                unread = jnp.logical_not(has_target(way))

                @pl.when(jnp.logical_and(unread, has_source(way, hop)))
                def _(way=way, hop=hop):
                    gathered(way, hop, i).wait_recv()


def per_device(params, first_moment, second_moment, grads, push_weight):
    replicas, shards = lax.axis_size("replica"), lax.axis_size("shard")
    _, rows, cols = params.shape
    units = cols // 128
    chunks = max(n for n in range(1, CHUNKS + 1) if units % n == 0)
    chunk = cols // chunks
    sub = max(128 * n for n in (1, 2) if chunk % (128 * n) == 0)
    plan = plan_of(replicas)
    rounds = len(plan)
    f32, bf16, dma = jnp.float32, jnp.bfloat16, pltpu.SemaphoreType.DMA
    anywhere = pl.BlockSpec(memory_space=pl.ANY)
    body = functools.partial(kernel, plan, replicas, shards, chunks, chunk, sub)
    hops = max(shards - 1, 1)
    return pl.pallas_call(
        body,
        out_shape=jax.ShapeDtypeStruct((1, rows * shards, cols), bf16),
        in_specs=[anywhere] * 4 + [pl.BlockSpec(memory_space=pltpu.SMEM)],
        out_specs=anywhere,
        scratch_shapes=[
            pltpu.VMEM((rows, cols), f32),
            pltpu.VMEM((rows, cols), f32),
            pltpu.VMEM((rows, cols), f32),
            pltpu.VMEM((STEPS, rows, cols), bf16),
            pltpu.VMEM((replicas, 8, 128), f32),
            pltpu.VMEM((STEPS + 2, rows, sub), f32),
            pltpu.VMEM((rows, cols), f32),
            pltpu.VMEM((max(rounds - 1, 1), rows, cols), f32),
            pltpu.VMEM((rounds, rows, cols), bf16),
            pltpu.VMEM((rounds, rows, cols), bf16),
            pltpu.VMEM((rows, cols), bf16),
            dma((4, chunks)),
            dma((replicas - 1,)),
            dma((replicas - 1,)),
            dma((rounds, chunks)),
            dma((rounds, chunks)),
            dma((2, hops, chunks)),
            dma((2, hops, chunks)),
            dma((chunks,)),
        ],
        compiler_params=pltpu.CompilerParams(
            collective_id=0, has_side_effects=True, vmem_limit_bytes=60 * 1024 * 1024
        ),
    )(params, first_moment, second_moment, grads, push_weight)


def solution(mesh):
    return jax.shard_map(
        per_device,
        mesh=mesh,
        in_specs=(
            P("replica", "shard", None),
            P("replica", "shard", None),
            P("replica", "shard", None),
            P(None, "replica", "shard", None),
            P("replica"),
        ),
        out_specs=P("replica", None, None),
        check_vma=False,
    )
```

```python
import functools

import jax
import jax.numpy as jnp
from jax import lax
from jax.experimental import pallas as pl
from jax.experimental.pallas import tpu as pltpu
from jax.sharding import PartitionSpec as P

STEPS = 4


beta_one = 0.9
beta_two = 0.95
learn_rate = 0.1
decay_rate = 0.1
epsilon = 1e-08
adam_offset = 101

CODE_SCALE = 8.0
LAG = 2
HOP_LAG = 2
CHUNKS = 28
LOAD_GROUP = 4
GATHER_GROUP = 1
MESH = pl.DeviceIdType.MESH


def plan_of(replicas):
    levels = replicas.bit_length() - 1
    distances = [2 ** (step % levels) for step in range(STEPS)]
    every = {2**level for level in range(levels)}
    plan = []
    for step, distance in enumerate(distances):
        later = set(distances[step + 1 :])
        if every <= later:
            continue
        above = {d for d in every if d > distance}
        plan.append((step, distance, above <= later))
    return plan


def encode(value):
    power = value * CODE_SCALE
    power = power * power
    power = power * power
    power = power * power
    power = power * power
    return jnp.where(value < 0.0, -power, power).astype(jnp.bfloat16)


def decode(code):
    code = code.astype(jnp.float32)
    size = jnp.exp(jnp.log(jnp.abs(code)) * (1.0 / 16.0)) * (1.0 / CODE_SCALE)
    return jnp.where(code < 0.0, -size, size)


def kernel(
    plan, replicas, shards, chunks, chunk, sub, load_group, gather_group,
    params_ref, first_ref, second_ref, grads_ref, weight_ref, out_ref,
    params, first, second, grads, weights, scales, acc, terms, sent, arrived, final,
    load_sem, wsend, wrecv, xsend, xrecv, zsend, zrecv, own_sem,
):
    me, z = lax.axis_index("replica"), lax.axis_index("shard")
    rows = params.shape[0]
    rounds = len(plan)
    keep = 1.0 - learn_rate * decay_rate

    def columns(i, group=1):
        return pl.ds(pl.multiple_of(i * (group * chunk), chunk), group * chunk)

    def slab(index):
        return pl.ds(pl.multiple_of(index * rows, rows), rows)

    def peer(offset):
        return lax.rem(me + offset + replicas, replicas)

    barrier = pltpu.get_barrier_semaphore()
    for k in range(1, replicas):
        pl.semaphore_signal(barrier, inc=1, device_id={"replica": peer(k)}, device_id_type=MESH)

    @pl.when(z > 0)
    def _():
        pl.semaphore_signal(barrier, inc=1, device_id={"shard": z - 1}, device_id_type=MESH)

    @pl.when(z < shards - 1)
    def _():
        pl.semaphore_signal(barrier, inc=1, device_id={"shard": z + 1}, device_id_type=MESH)

    def loads(i):
        cols = columns(i, load_group)
        return (
            pltpu.make_async_copy(params_ref.at[0, :, cols], params.at[:, cols], load_sem.at[0, i]),
            pltpu.make_async_copy(first_ref.at[0, :, cols], first.at[:, cols], load_sem.at[1, i]),
            pltpu.make_async_copy(second_ref.at[0, :, cols], second.at[:, cols], load_sem.at[2, i]),
            pltpu.make_async_copy(grads_ref.at[:, 0, :, cols], grads.at[:, :, cols], load_sem.at[3, i]),
        )

    @pl.loop(0, chunks // load_group)
    def _(i):
        for copy in loads(i):
            copy.start()

    weights[me] = jnp.full(weights.shape[1:], weight_ref[0], jnp.float32)
    ends_of_line = jnp.where(z > 0, 1, 0) + jnp.where(z < shards - 1, 1, 0)
    pl.semaphore_wait(barrier, replicas - 1 + ends_of_line)

    def weight_copy(k, owner):
        return pltpu.make_async_remote_copy(
            src_ref=weights.at[owner], dst_ref=weights.at[owner],
            send_sem=wsend.at[k - 1], recv_sem=wrecv.at[k - 1],
            device_id={"replica": peer(k)}, device_id_type=MESH,
        )

    for k in range(1, replicas):
        weight_copy(k, me).start()
    for k in range(1, replicas):
        weight_copy(k, peer(-k)).wait_recv()

    def wide(tile):
        tile = jnp.concatenate([tile] * (rows // tile.shape[0]), axis=0) if rows > tile.shape[0] else tile[:rows]
        return jnp.concatenate([tile] * (sub // tile.shape[1]), axis=1)

    levels = replicas.bit_length() - 1
    behind = [weights[peer(-k)] for k in range(replicas)]
    ends = [step for step, _, _ in plan]
    for step in range(STEPS):
        end = min(e for e in ends if e >= step)
        if step == 0:
            scales[0] = wide(behind[0] * keep ** (end + 1))
        scales[1 + step] = wide(behind[0] * (learn_rate * keep ** (end - step)))
        distance = 2 ** (step % levels)
        behind = [0.5 * behind[k] + 0.5 * behind[(k + distance) % replicas] for k in range(replicas)]
    scales[1 + STEPS] = wide(0.5 / behind[0])

    def exchange(k, i):
        _, distance, swap = plan[k]
        if swap:
            to = me + distance - 2 * distance * lax.rem(me // distance, 2)
        else:
            to = peer(distance)
        cols = slice(None) if i is None else columns(i)
        return pltpu.make_async_remote_copy(
            src_ref=sent.at[k, :, cols], dst_ref=arrived.at[k, :, cols],
            send_sem=xsend.at[k], recv_sem=xrecv.at[k, 0 if i is None else i],
            device_id={"replica": to}, device_id_type=MESH,
        )

    def gather(way, hop, i):
        sign = 1 - 2 * way
        cols, index = slice(None) if i is None else columns(i, gather_group), z - sign * hop
        target = out_ref.at[0, slab(index), cols]
        return pltpu.make_async_remote_copy(
            src_ref=final.at[:, cols] if hop == 0 else target, dst_ref=target,
            send_sem=zsend.at[way, hop], recv_sem=zrecv.at[way, hop, 0 if i is None else i],
            device_id={"shard": z + sign}, device_id_type=MESH,
        )

    def gathered(way, hop, i):
        sign = 1 - 2 * way
        target = out_ref.at[0, slab(z - sign * hop), columns(i, gather_group)]
        return pltpu.make_async_remote_copy(
            src_ref=target, dst_ref=target,
            send_sem=zsend.at[way, hop - 1], recv_sem=zrecv.at[way, hop - 1, i],
            device_id={"shard": z - sign}, device_id_type=MESH,
        )

    def has_source(way, hop):
        return z >= hop if way == 0 else z + hop < shards

    def has_target(way):
        return z < shards - 1 if way == 0 else z > 0

    def own(i):
        cols = slice(None) if i is None else columns(i, gather_group)
        return pltpu.make_async_copy(final.at[:, cols], out_ref.at[0, slab(z), cols], own_sem)

    def start_round(i):
        @pl.when(lax.rem(i, load_group) == 0)
        def _():
            for copy in loads(i // load_group):
                copy.wait()

        for j in range(chunk // sub):
            cols = pl.ds(pl.multiple_of(i * chunk + j * sub, sub), sub)
            m, v = first[:, cols], second[:, cols]
            total = scales[0] * params[:, cols]
            k = 0
            for step in range(STEPS):
                g = grads[step, :, cols].astype(jnp.float32)
                count = adam_offset + step
                m = beta_one * m + (1.0 - beta_one) * g
                v = beta_two * v + (1.0 - beta_two) * g * g
                fixed = jnp.sqrt(v * (1.0 / (1.0 - beta_two**count))) + epsilon
                update = m * (1.0 / (1.0 - beta_one**count)) / fixed * scales[1 + step]
                total = -update if total is None else total - update
                if step == ends[k]:
                    if k == 0:
                        acc[:, cols] = total
                        sent[0, :, cols] = encode(total)
                    else:
                        terms[k - 1, :, cols] = total
                    total, k = None, k + 1
        exchange(0, i).start()

    def next_round(k, i):
        exchange(k - 1, i).wait_recv()
        for j in range(chunk // sub):
            cols = pl.ds(pl.multiple_of(i * chunk + j * sub, sub), sub)
            both = acc[:, cols] + decode(arrived[k - 1, :, cols])
            if k < rounds:
                both = both * (0.5 * keep ** (ends[k] - ends[k - 1])) + terms[k - 1, :, cols]
                acc[:, cols] = both
                sent[k, :, cols] = encode(both)
            else:
                final[:, cols] = (both * scales[1 + STEPS]).astype(jnp.bfloat16)
        if k < rounds:
            exchange(k, i).start()
        else:

            @pl.when(lax.rem(i, gather_group) == gather_group - 1)
            def _():
                for way in range(2):
                    pl.when(has_target(way))(lambda way=way: gather(way, 0, i // gather_group).start())
                own(i // gather_group).start()

    def pass_on(hop, i):
        for way in range(2):

            whole = lax.rem(i, gather_group) == gather_group - 1

            @pl.when(jnp.logical_and(whole, jnp.logical_and(has_target(way), has_source(way, hop))))
            def _(way=way):
                gathered(way, hop, i // gather_group).wait_recv()
                gather(way, hop, i // gather_group).start()

    hops = shards - 2

    @pl.loop(0, chunks + rounds * LAG + max(hops, 0) * HOP_LAG)
    def _(t):
        def at(delay, act):
            i = t - delay

            @pl.when(jnp.logical_and(i >= 0, i < chunks))
            def _():
                act(i)

        at(0, start_round)
        for k in range(1, rounds + 1):
            at(k * LAG, functools.partial(next_round, k))
        for hop in range(1, hops + 1):
            at(rounds * LAG + hop * HOP_LAG, functools.partial(pass_on, hop))

    for way in range(2):

        @pl.when(jnp.logical_not(has_target(way)))
        def _(way=way):
            @pl.loop(0, chunks // gather_group)
            def _(i):
                for hop in range(1, shards):
                    pl.when(has_source(way, hop))(lambda hop=hop: gathered(way, hop, i).wait_recv())

    for k in range(1, replicas):
        weight_copy(k, me).wait_send()
    for k in range(rounds):
        exchange(k, None).wait_send()
    own(None).wait()
    for way in range(2):
        for hop in range(shards - 1):

            @pl.when(jnp.logical_and(has_target(way), has_source(way, hop)))
            def _(way=way, hop=hop):
                gather(way, hop, None).wait_send()


def per_device(params, first_moment, second_moment, grads, push_weight):
    replicas, shards = lax.axis_size("replica"), lax.axis_size("shard")
    _, rows, cols = params.shape
    units = cols // 128
    chunks = max(n for n in range(1, CHUNKS + 1) if units % n == 0)
    chunk = cols // chunks
    sub = max(128 * n for n in (1, 2) if chunk % (128 * n) == 0)
    load_group = LOAD_GROUP if chunks % LOAD_GROUP == 0 else 1
    gather_group = GATHER_GROUP if chunks % GATHER_GROUP == 0 else 1
    plan = plan_of(replicas)
    rounds = len(plan)
    f32, bf16, dma = jnp.float32, jnp.bfloat16, pltpu.SemaphoreType.DMA
    anywhere = pl.BlockSpec(memory_space=pl.ANY)
    body = functools.partial(kernel, plan, replicas, shards, chunks, chunk, sub, load_group, gather_group)
    hops = max(shards - 1, 1)
    large = (params, first_moment, second_moment, grads)
    large = tuple(pltpu.with_memory_space_constraint(x, pltpu.HBM) for x in large)
    return pl.pallas_call(
        body,
        out_shape=jax.ShapeDtypeStruct((1, rows * shards, cols), bf16),
        in_specs=[anywhere] * 4 + [pl.BlockSpec(memory_space=pltpu.SMEM)],
        out_specs=anywhere,
        scratch_shapes=[
            pltpu.VMEM((rows, cols), f32),
            pltpu.VMEM((rows, cols), f32),
            pltpu.VMEM((rows, cols), f32),
            pltpu.VMEM((STEPS, rows, cols), bf16),
            pltpu.VMEM((replicas, 8, 128), f32),
            pltpu.VMEM((STEPS + 2, rows, sub), f32),
            pltpu.VMEM((rows, cols), f32),
            pltpu.VMEM((max(rounds - 1, 1), rows, cols), f32),
            pltpu.VMEM((rounds, rows, cols), bf16),
            pltpu.VMEM((rounds, rows, cols), bf16),
            pltpu.VMEM((rows, cols), bf16),
            dma((4, chunks // load_group)),
            dma((replicas - 1,)),
            dma((replicas - 1,)),
            dma((rounds,)),
            dma((rounds, chunks)),
            dma((2, hops)),
            dma((2, hops, chunks // gather_group)),
            dma,
        ],
        compiler_params=pltpu.CompilerParams(
            collective_id=0, has_side_effects=True, vmem_limit_bytes=48 * 1024 * 1024
        ),
    )(*large, push_weight)


def solution(mesh):
    return jax.shard_map(
        per_device,
        mesh=mesh,
        in_specs=(
            P("replica", "shard", None),
            P("replica", "shard", None),
            P("replica", "shard", None),
            P(None, "replica", "shard", None),
            P("replica"),
        ),
        out_specs=P("replica", None, None),
        check_vma=False,
    )
```

```python
import functools

import jax
import jax.numpy as jnp
from jax import lax
from jax.experimental import pallas as pl
from jax.experimental.pallas import tpu as pltpu
from jax.sharding import PartitionSpec as P

STEPS = 4


beta_one = 0.9
beta_two = 0.95
learn_rate = 0.1
decay_rate = 0.1
epsilon = 1e-08
adam_offset = 101

CODE_SCALE = 8.0
LAG = 3
HOP_LAG = 3
CHUNKS = 28
LOAD_GROUP = 2
GATHER_GROUP = 1
MESH = pl.DeviceIdType.MESH


def plan_of(replicas):
    levels = replicas.bit_length() - 1
    distances = [2 ** (step % levels) for step in range(STEPS)]
    every = {2**level for level in range(levels)}
    plan = []
    for step, distance in enumerate(distances):
        later = set(distances[step + 1 :])
        if every <= later:
            continue
        above = {d for d in every if d > distance}
        plan.append((step, distance, above <= later))
    return plan


def encode(value):
    power = value * CODE_SCALE
    power = power * power
    power = power * power
    power = power * power
    power = power * power
    return jnp.where(value < 0.0, -power, power).astype(jnp.bfloat16)


def decode(code):
    code = code.astype(jnp.float32)
    size = jnp.exp(jnp.log(jnp.abs(code)) * (1.0 / 16.0)) * (1.0 / CODE_SCALE)
    return jnp.where(code < 0.0, -size, size)


def kernel(
    plan, replicas, shards, chunks, chunk, sub, load_group, gather_group,
    params_ref, first_ref, second_ref, grads_ref, weight_ref, out_ref,
    params, first, second, grads, weights, scales, acc, terms, sent, arrived, final,
    load_sem, wsend, wrecv, xsend, xrecv, zsend, zrecv, own_sem,
):
    me, z = lax.axis_index("replica"), lax.axis_index("shard")
    rows = params.shape[0]
    rounds = len(plan)
    keep = 1.0 - learn_rate * decay_rate

    def columns(i, group=1):
        return pl.ds(pl.multiple_of(i * (group * chunk), chunk), group * chunk)

    def slab(index):
        return pl.ds(pl.multiple_of(index * rows, rows), rows)

    def peer(offset):
        return lax.rem(me + offset + replicas, replicas)

    barrier = pltpu.get_barrier_semaphore()
    for k in range(1, replicas):
        pl.semaphore_signal(barrier, inc=1, device_id={"replica": peer(k)}, device_id_type=MESH)

    @pl.when(z > 0)
    def _():
        pl.semaphore_signal(barrier, inc=1, device_id={"shard": z - 1}, device_id_type=MESH)

    @pl.when(z < shards - 1)
    def _():
        pl.semaphore_signal(barrier, inc=1, device_id={"shard": z + 1}, device_id_type=MESH)

    def loads(i):
        cols = columns(i, load_group)
        return (
            pltpu.make_async_copy(params_ref.at[0, :, cols], params.at[:, cols], load_sem.at[0, i]),
            pltpu.make_async_copy(first_ref.at[0, :, cols], first.at[:, cols], load_sem.at[1, i]),
            pltpu.make_async_copy(second_ref.at[0, :, cols], second.at[:, cols], load_sem.at[2, i]),
            pltpu.make_async_copy(grads_ref.at[:, 0, :, cols], grads.at[:, :, cols], load_sem.at[3, i]),
        )

    @pl.loop(0, chunks // load_group)
    def _(i):
        for copy in loads(i):
            copy.start()

    weights[me] = jnp.full(weights.shape[1:], weight_ref[0], jnp.float32)
    ends_of_line = jnp.where(z > 0, 1, 0) + jnp.where(z < shards - 1, 1, 0)
    pl.semaphore_wait(barrier, replicas - 1 + ends_of_line)

    def weight_copy(k, owner):
        return pltpu.make_async_remote_copy(
            src_ref=weights.at[owner], dst_ref=weights.at[owner],
            send_sem=wsend.at[k - 1], recv_sem=wrecv.at[k - 1],
            device_id={"replica": peer(k)}, device_id_type=MESH,
        )

    for k in range(1, replicas):
        weight_copy(k, me).start()
    for k in range(1, replicas):
        weight_copy(k, peer(-k)).wait_recv()

    def wide(tile):
        tile = jnp.concatenate([tile] * (rows // tile.shape[0]), axis=0) if rows > tile.shape[0] else tile[:rows]
        return jnp.concatenate([tile] * (sub // tile.shape[1]), axis=1)

    levels = replicas.bit_length() - 1
    behind = [weights[peer(-k)] for k in range(replicas)]
    ends = [step for step, _, _ in plan]
    for step in range(STEPS):
        end = min(e for e in ends if e >= step)
        if step == 0:
            scales[0] = wide(behind[0] * keep ** (end + 1))
        scales[1 + step] = wide(behind[0] * (learn_rate * keep ** (end - step)))
        distance = 2 ** (step % levels)
        behind = [0.5 * behind[k] + 0.5 * behind[(k + distance) % replicas] for k in range(replicas)]
    scales[1 + STEPS] = wide(0.5 / behind[0])

    def exchange(k, i):
        _, distance, swap = plan[k]
        if swap:
            to = me + distance - 2 * distance * lax.rem(me // distance, 2)
        else:
            to = peer(distance)
        cols = slice(None) if i is None else columns(i)
        return pltpu.make_async_remote_copy(
            src_ref=sent.at[k, :, cols], dst_ref=arrived.at[k, :, cols],
            send_sem=xsend.at[k], recv_sem=xrecv.at[k, 0 if i is None else i],
            device_id={"replica": to}, device_id_type=MESH,
        )

    def gather(way, hop, i):
        sign = 1 - 2 * way
        cols, index = slice(None) if i is None else columns(i, gather_group), z - sign * hop
        target = out_ref.at[0, slab(index), cols]
        return pltpu.make_async_remote_copy(
            src_ref=final.at[:, cols] if hop == 0 else target, dst_ref=target,
            send_sem=zsend.at[way, hop], recv_sem=zrecv.at[way, hop, 0 if i is None else i],
            device_id={"shard": z + sign}, device_id_type=MESH,
        )

    def gathered(way, hop, i):
        sign = 1 - 2 * way
        target = out_ref.at[0, slab(z - sign * hop), columns(i, gather_group)]
        return pltpu.make_async_remote_copy(
            src_ref=target, dst_ref=target,
            send_sem=zsend.at[way, hop - 1], recv_sem=zrecv.at[way, hop - 1, i],
            device_id={"shard": z - sign}, device_id_type=MESH,
        )

    def has_source(way, hop):
        return z >= hop if way == 0 else z + hop < shards

    def has_target(way):
        return z < shards - 1 if way == 0 else z > 0

    def own(i):
        cols = slice(None) if i is None else columns(i, gather_group)
        return pltpu.make_async_copy(final.at[:, cols], out_ref.at[0, slab(z), cols], own_sem)

    def start_round(i):
        @pl.when(lax.rem(i, load_group) == 0)
        def _():
            for copy in loads(i // load_group):
                copy.wait()

        for j in range(chunk // sub):
            cols = pl.ds(pl.multiple_of(i * chunk + j * sub, sub), sub)
            m, v = first[:, cols], second[:, cols]
            total = scales[0] * params[:, cols]
            k = 0
            for step in range(STEPS):
                g = grads[step, :, cols].astype(jnp.float32)
                count = adam_offset + step
                m = beta_one * m + (1.0 - beta_one) * g
                v = beta_two * v + (1.0 - beta_two) * g * g
                fixed = jnp.sqrt(v * (1.0 / (1.0 - beta_two**count))) + epsilon
                update = m * (1.0 / (1.0 - beta_one**count)) / fixed * scales[1 + step]
                total = -update if total is None else total - update
                if step == ends[k]:
                    if k == 0:
                        acc[:, cols] = total
                        sent[0, :, cols] = encode(total)
                    else:
                        terms[k - 1, :, cols] = total
                    total, k = None, k + 1
        exchange(0, i).start()

    def next_round(k, i):
        exchange(k - 1, i).wait_recv()
        for j in range(chunk // sub):
            cols = pl.ds(pl.multiple_of(i * chunk + j * sub, sub), sub)
            both = acc[:, cols] + decode(arrived[k - 1, :, cols])
            if k < rounds:
                both = both * (0.5 * keep ** (ends[k] - ends[k - 1])) + terms[k - 1, :, cols]
                acc[:, cols] = both
                sent[k, :, cols] = encode(both)
            else:
                final[:, cols] = (both * scales[1 + STEPS]).astype(jnp.bfloat16)
        if k < rounds:
            exchange(k, i).start()
        else:

            @pl.when(lax.rem(i, gather_group) == gather_group - 1)
            def _():
                for way in range(2):
                    pl.when(has_target(way))(lambda way=way: gather(way, 0, i // gather_group).start())
                own(i // gather_group).start()

    def pass_on(hop, i):
        for way in range(2):

            whole = lax.rem(i, gather_group) == gather_group - 1

            @pl.when(jnp.logical_and(whole, jnp.logical_and(has_target(way), has_source(way, hop))))
            def _(way=way):
                gathered(way, hop, i // gather_group).wait_recv()
                gather(way, hop, i // gather_group).start()

    hops = shards - 2

    @pl.loop(0, chunks + rounds * LAG + max(hops, 0) * HOP_LAG)
    def _(t):
        def at(delay, act):
            i = t - delay

            @pl.when(jnp.logical_and(i >= 0, i < chunks))
            def _():
                act(i)

        at(0, start_round)
        for k in range(1, rounds + 1):
            at(k * LAG, functools.partial(next_round, k))
        for hop in range(1, hops + 1):
            at(rounds * LAG + hop * HOP_LAG, functools.partial(pass_on, hop))

    for way in range(2):

        @pl.when(jnp.logical_not(has_target(way)))
        def _(way=way):
            @pl.loop(0, chunks // gather_group)
            def _(i):
                for hop in range(1, shards):
                    pl.when(has_source(way, hop))(lambda hop=hop: gathered(way, hop, i).wait_recv())

    for k in range(1, replicas):
        weight_copy(k, me).wait_send()
    for k in range(rounds):
        exchange(k, None).wait_send()
    own(None).wait()
    for way in range(2):
        for hop in range(shards - 1):

            @pl.when(jnp.logical_and(has_target(way), has_source(way, hop)))
            def _(way=way, hop=hop):
                gather(way, hop, None).wait_send()


def per_device(params, first_moment, second_moment, grads, push_weight):
    replicas, shards = lax.axis_size("replica"), lax.axis_size("shard")
    _, rows, cols = params.shape
    units = cols // 128
    chunks = max(n for n in range(1, CHUNKS + 1) if units % n == 0)
    chunk = cols // chunks
    sub = max(128 * n for n in (1, 2) if chunk % (128 * n) == 0)
    load_group = LOAD_GROUP if chunks % LOAD_GROUP == 0 else 1
    gather_group = GATHER_GROUP if chunks % GATHER_GROUP == 0 else 1
    plan = plan_of(replicas)
    rounds = len(plan)
    f32, bf16, dma = jnp.float32, jnp.bfloat16, pltpu.SemaphoreType.DMA
    anywhere = pl.BlockSpec(memory_space=pl.ANY)
    body = functools.partial(kernel, plan, replicas, shards, chunks, chunk, sub, load_group, gather_group)
    hops = max(shards - 1, 1)
    large = (params, first_moment, second_moment, grads)
    large = tuple(pltpu.with_memory_space_constraint(x, pltpu.HBM) for x in large)
    return pl.pallas_call(
        body,
        out_shape=jax.ShapeDtypeStruct((1, rows * shards, cols), bf16),
        in_specs=[anywhere] * 4 + [pl.BlockSpec(memory_space=pltpu.SMEM)],
        out_specs=anywhere,
        scratch_shapes=[
            pltpu.VMEM((rows, cols), f32),
            pltpu.VMEM((rows, cols), f32),
            pltpu.VMEM((rows, cols), f32),
            pltpu.VMEM((STEPS, rows, cols), bf16),
            pltpu.VMEM((replicas, 8, 128), f32),
            pltpu.VMEM((STEPS + 2, rows, sub), f32),
            pltpu.VMEM((rows, cols), f32),
            pltpu.VMEM((max(rounds - 1, 1), rows, cols), f32),
            pltpu.VMEM((rounds, rows, cols), bf16),
            pltpu.VMEM((rounds, rows, cols), bf16),
            pltpu.VMEM((rows, cols), bf16),
            dma((4, chunks // load_group)),
            dma((replicas - 1,)),
            dma((replicas - 1,)),
            dma((rounds,)),
            dma((rounds, chunks)),
            dma((2, hops)),
            dma((2, hops, chunks // gather_group)),
            dma,
        ],
        compiler_params=pltpu.CompilerParams(
            collective_id=0, has_side_effects=True, vmem_limit_bytes=48 * 1024 * 1024
        ),
    )(*large, push_weight)


def solution(mesh):
    return jax.shard_map(
        per_device,
        mesh=mesh,
        in_specs=(
            P("replica", "shard", None),
            P("replica", "shard", None),
            P("replica", "shard", None),
            P(None, "replica", "shard", None),
            P("replica"),
        ),
        out_specs=P("replica", None, None),
        check_vma=False,
    )
```
